32 devices in a mesh: dp: 2 (over core), rows: 4 (over y, x), heads: 4 (over z).
Axes of the slice: x: 2, y: 2, z: 4, core: 2. Of those that a mesh axis runs over, the one named last changes fastest.
Arguments:
- hidden: bfloat16 [2, 16, 2048], P('dp'), may hold values from -458.54834 to 458.54834
- norm_gain: float32 [1, 2048], replicated, may hold values from 0.25 to 1.75
- query_weight: bfloat16 [1, 2048, 4096], P(None, None, ('heads', 'rows')), may hold values from -0.125 to 0.125
- key_weight: bfloat16 [1, 2048, 4096], P(None, None, ('heads', 'rows')), may hold values from -0.125 to 0.125
- value_weight: bfloat16 [1, 2048, 4096], P(None, None, ('heads', 'rows')), may hold values from -0.125 to 0.125
- zgate_weight: bfloat16 [1, 2048, 4096], P(None, None, ('heads', 'rows')), may hold values from -0.125 to 0.125
- gate_weight: bfloat16 [1, 2, 2048, 4], P(None, None, None, 'heads'), may hold values from -0.125 to 0.125
- decay_rate: float32 [1, 4], P(None, 'heads'), may hold values from 0.005 to 0.5
- output_gain: float32 [1, 1024], P(None, 'rows'), may hold values from 0.25 to 1.75
- output_weight: bfloat16 [1, 4096, 2048], P(None, ('heads', 'rows')), may hold values from -0.09375 to 0.09375
- recurrent_state: float32 [1, 2, 4, 1024, 1024], P(None, 'dp', 'heads', 'rows'), may hold values from -6 to 6
- final_gain: float32 [2048], replicated, may hold values from 0.25 to 1.75
- vocab_weight: bfloat16 [2048, 131072], P(None, ('dp', 'rows', 'heads')), may hold values from -7.9549513 to 7.9549513
Outputs:
- next_state: float32 [1, 2, 4, 1024, 1024], P(None, 'dp', 'heads', 'rows')
- log_probs: float32 [2, 16, 131072], P(None, None, ('dp', 'rows', 'heads'))
The draws below stay inside these ranges and needn't reach their ends.
All inputs are finite; a program needn't handle non-finite values.
Results may differ from the reference program's by a relative error of at most 0.0024.
The reference program's roundings to bfloat16 on the way (of `normed_in`, `gated` and `final_in`) count: a program that leaves them out, or rounds other values in their place, can miss the bound.
Values may be sent and summed in bfloat16 or wider, within the bound.
A program may use at most 64 MiB of HBM per device.

```python
import math
import jax
import jax.numpy as jnp
from jax import lax

D = 2048
H = 4
DK = 1024
DV = 1024
LAYERS = 1
TOKS = 16
V = 131072
SEQS = 2


def loud_feature(key):
    return jax.random.randint(jax.random.fold_in(key, 911), (), 0, D)


def draw_hidden(key, part):
    loud = loud_feature(key)
    keys = jax.random.split(jax.random.fold_in(key, 17), 4)
    base = jnp.clip(jax.random.normal(keys[0], (SEQS, TOKS, D), jnp.float32), -6.0, 6.0)
    picked = jax.random.randint(keys[1], (SEQS, TOKS), 0, 4) == 0
    picked = jnp.logical_or(picked, (jnp.arange(TOKS) == 0)[None, :])
    amount = jnp.exp(jax.random.uniform(keys[2], (SEQS, TOKS), jnp.float32, math.log(3.0), math.log(10.0))) * math.sqrt(D)
    signs = jnp.where(jax.random.randint(keys[3], (SEQS, TOKS), 0, 2) == 0, -1.0, 1.0)
    spike = jnp.where(picked, amount * signs, 0.0)
    onehot = (jnp.arange(D) == loud).astype(jnp.float32)
    return (base + spike[..., None] * onehot).astype(jnp.bfloat16)


def draw_vocab_weight(key, part):
    loud = loud_feature(key)
    keys = jax.random.split(jax.random.fold_in(key, 23), 2)
    base = jnp.clip(jax.random.normal(keys[0], (D, V), jnp.float32), -6.0, 6.0)
    loud_row = jnp.clip(jax.random.normal(keys[1], (1, V), jnp.float32), -6.0, 6.0)
    drawn = base * (D / 9.0) ** (-0.5)
    strong = loud_row * (60.0 / math.sqrt(D))
    chosen = (jnp.arange(D) == loud)[:, None]
    return jnp.where(chosen, strong, drawn).astype(jnp.bfloat16)


def level_of(key, dims, cuts, least, largest):
    level = 1.0
    for dim, parts in cuts:
        steps = jax.random.uniform(jax.random.fold_in(jax.random.fold_in(key, 6), dim), (parts,), jnp.float32, least / len(cuts), largest / len(cuts))
        level = level * jnp.repeat(jnp.exp(steps), dims[dim] // parts).reshape((-1,) + (1,) * (len(dims) - 1 - dim))
    return level


def centred(stream_key, dims, deviation, reach, cuts=(), held_as=jnp.bfloat16):
    entries = jax.random.normal(stream_key, dims, jnp.float32) * deviation
    if len(cuts) > 0:
        entries = level_of(stream_key, dims, cuts, -0.22, 0.18) * entries
    return jnp.clip(entries, min=-reach, max=reach).astype(held_as)


def setup_inputs(seed: int = 0) -> dict:
    splits = jax.random.split(jax.random.key(seed), 14)
    return {
        "hidden": draw_hidden(jax.random.fold_in(splits[13], 71), 0),
        "norm_gain": jnp.clip(1.0 + 0.15 * jax.random.normal(splits[1], (LAYERS, D), jnp.float32), 0.25, 1.75),
        "query_weight": centred(splits[2], (LAYERS, D, H * DK), D ** -0.5, 0.125, ((2, 16),)),
        "key_weight": centred(splits[3], (LAYERS, D, H * DK), D ** -0.5, 0.125, ((2, 16),)),
        "value_weight": centred(splits[4], (LAYERS, D, H * DV), D ** -0.5, 0.125, ((2, 16),)),
        "zgate_weight": centred(splits[5], (LAYERS, D, H * DV), D ** -0.5, 0.125, ((2, 16),)),
        "gate_weight": centred(splits[6], (LAYERS, 2, D, H), D ** -0.5, 0.125, ((3, 4),)),
        "decay_rate": jnp.clip(jnp.exp(math.log(0.5) - 4.6051702 * jax.random.uniform(splits[7], (LAYERS, H), jnp.float32) ** level_of(splits[7], (LAYERS, H), ((1, 4),), -0.2, 0.2)), 0.005, 0.5),
        "output_gain": jnp.clip(1.0 + 0.15 * jax.random.normal(splits[8], (LAYERS, DV), jnp.float32), 0.25, 1.75),
        "output_weight": centred(splits[9], (LAYERS, H * DV, D), (H * DV) ** -0.5, 0.09375, ((1, 16),)),
        "recurrent_state": centred(splits[10], (LAYERS, SEQS, H, DK, DV), 1.0, 6.0, ((1, 2), (2, 4), (3, 4)), jnp.float32),
        "final_gain": jnp.clip(1.0 + 0.15 * jax.random.normal(splits[11], (D,), jnp.float32), 0.25, 1.75),
        "vocab_weight": draw_vocab_weight(jax.random.fold_in(splits[13], 71), 0),
    }


epsilon = 1e-06

def rms_norm(values, gain):
    return values * lax.rsqrt(lax.optimization_barrier(jnp.mean(values * values, axis=-1, keepdims=True)) + epsilon) * gain

def reference(hidden, norm_gain, query_weight, key_weight, value_weight, zgate_weight, gate_weight, decay_rate, output_gain, output_weight, recurrent_state, final_gain, vocab_weight):
    highest_score = lax.Precision.HIGHEST
    stream = hidden.astype(jnp.float32)
    states_out = []
    for layer_idx in range(LAYERS):
        normed_in = rms_norm(stream, norm_gain[layer_idx]).astype(jnp.bfloat16)
        flat = normed_in.reshape(-1, D)

        def project(weight, size):
            return jnp.dot(flat, weight[layer_idx], preferred_element_type=jnp.float32).reshape(SEQS, TOKS, H, size)
        query = project(query_weight, DK)
        key = project(key_weight, DK)
        value = project(value_weight, DV)
        zgate = project(zgate_weight, DV)
        gates = jnp.einsum('md,gdh->gmh', flat.astype(jnp.float32), gate_weight[layer_idx].astype(jnp.float32), precision=highest_score)
        gates = gates.reshape(2, SEQS, TOKS, H)
        log_decay = -decay_rate[layer_idx] * jax.nn.softplus(gates[0])
        strength = jax.nn.sigmoid(gates[1])
        query = query * lax.rsqrt(lax.optimization_barrier(jnp.sum(query * query, axis=-1, keepdims=True)) + epsilon) * DK ** (-0.5)
        key = key * lax.rsqrt(lax.optimization_barrier(jnp.sum(key * key, axis=-1, keepdims=True)) + epsilon)

        def advance(carry, inputs):
            query_t, key_t, value_t, decay_t, strength_t = inputs
            carry = jnp.exp(decay_t)[..., None, None] * carry
            guess = jnp.einsum('shk,shkv->shv', key_t, carry, precision=highest_score)
            update = strength_t[..., None] * (value_t - guess)
            carry = carry + key_t[..., :, None] * update[..., None, :]
            readout = jnp.einsum('shk,shkv->shv', query_t, carry, precision=highest_score)
            return (carry, readout)
        inputs = tuple((jnp.moveaxis(item, 1, 0) for item in (query, key, value, log_decay, strength)))
        final_state, readouts = lax.scan(advance, recurrent_state[layer_idx], inputs)
        readouts = jnp.moveaxis(readouts, 0, 1)
        gated = (rms_norm(readouts, output_gain[layer_idx]) * jax.nn.silu(zgate)).astype(jnp.bfloat16)
        mixed = jnp.dot(gated.reshape(-1, H * DV), output_weight[layer_idx], preferred_element_type=jnp.float32)
        stream = stream + mixed.reshape(SEQS, TOKS, D)
        states_out.append(final_state)
    final_in = rms_norm(stream, final_gain).astype(jnp.bfloat16)
    logits = jnp.dot(final_in.reshape(-1, D), vocab_weight, preferred_element_type=jnp.float32)
    row_peak = lax.optimization_barrier(jnp.max(logits, axis=-1, keepdims=True))
    log_total = row_peak + jnp.log(lax.optimization_barrier(jnp.sum(jnp.exp(logits - row_peak), axis=-1, keepdims=True)))
    log_probs = (logits - log_total).reshape(SEQS, TOKS, V)
    return (jnp.stack(states_out), log_probs)
```

```python
import functools

import jax
import jax.numpy as jnp
from jax import lax
from jax.experimental import pallas as pl
from jax.experimental.pallas import tpu as pltpu
from jax.sharding import PartitionSpec as P

MESH = pl.DeviceIdType.MESH
f32 = jnp.float32
bf16 = jnp.bfloat16
epsilon = 1e-06
HIGHEST = lax.Precision.HIGHEST
LANES = 128


def halves(x):
    high = x.astype(bf16)
    return high, (x - high.astype(f32)).astype(bf16)


def dot(a, b, dims=((1,), (0,)), precision=None):
    return lax.dot_general(a, b, (dims, ((), ())), precision=precision, preferred_element_type=f32)


def exchange(n, me, src_of, dst, send, recv, device_of):
    def other(k):
        return lax.rem(me + k, n)

    def outgoing(p):
        return pltpu.make_async_remote_copy(
            src_ref=src_of(p), dst_ref=dst.at[me], send_sem=send.at[p], recv_sem=recv.at[me],
            device_id=device_of(p), device_id_type=MESH)

    def incoming(p):
        return pltpu.make_async_remote_copy(
            src_ref=dst.at[p], dst_ref=dst.at[p], send_sem=send.at[p], recv_sem=recv.at[p],
            device_id=device_of(p), device_id_type=MESH)

    def over(act):
        def step(k, _):
            act(other(k))
            return 0

        lax.fori_loop(1, n, step, 0)

    over(lambda p: outgoing(p).start())
    return (lambda: over(lambda p: incoming(p).wait_recv()),
            lambda: over(lambda p: outgoing(p).wait_send()))


def kernel(shape, chunks,
           hidden, norm_gain, qw, kw, vw, zw, gw, rate, ogain, ow, state, fgain, vocab,
           new_state, logits_out, total_out,
           hid_v, ngain_v, qw_v, kw_v, vw_v, zw_v, gw_v, rate_v, ogain_v, ow_v, state_v, fgain_v, voc_v,
           aux, look, read_v, parts, rs, ag, fin, stats, ns_v, log_v, tot_v,
           in_sem, voc_sem, out_sem,
           aux_s, aux_r, look_s, look_r, rs_s, rs_r, ag_s, ag_r, fin_s, fin_r, st_s, st_r):
    dps, rows, heads = shape["dp"], shape["rows"], shape["heads"]
    group = rows * heads
    everyone = dps * group
    d, r, h = (lax.axis_index(a) for a in ("dp", "rows", "heads"))
    g = r * heads + h
    me = d * group + g
    tokens, width = hid_v.shape
    vs = vw_v.shape[1]

    def in_group(p):
        return {"dp": d, "rows": lax.div(p, heads), "heads": lax.rem(p, heads)}

    def anywhere(p):
        q = lax.rem(p, group)
        return {"dp": lax.div(p, group), "rows": lax.div(q, heads), "heads": lax.rem(q, heads)}

    def in_rows(p):
        return {"dp": d, "rows": p, "heads": h}

    def in_dp(p):
        return {"dp": p, "rows": r, "heads": h}

    loads = {}
    order = (("hid", hidden, hid_v), ("ngain", norm_gain, ngain_v), ("kw", kw, kw_v), ("qw", qw, qw_v),
             ("vw", vw, vw_v), ("state", state, state_v), ("gw", gw, gw_v), ("rate", rate, rate_v),
             ("zw", zw, zw_v), ("ogain", ogain, ogain_v), ("fgain", fgain, fgain_v), ("ow", ow, ow_v))
    for i, (name, src, dst) in enumerate(order):
        loads[name] = pltpu.make_async_copy(src, dst, in_sem.at[i])
        loads[name].start()
    barrier = pltpu.get_barrier_semaphore()

    def greet(k, _):
        pl.semaphore_signal(barrier, inc=1, device_id=anywhere(lax.rem(me + k, everyone)), device_id_type=MESH)
        return 0

    lax.fori_loop(1, everyone, greet, 0)

    loads["hid"].wait()
    loads["ngain"].wait()
    stream = hid_v[...].astype(f32)
    normed = (stream * lax.rsqrt(jnp.mean(stream * stream, axis=-1, keepdims=True) + epsilon) * ngain_v[...]).astype(bf16)
    loads["kw"].wait()
    key = dot(normed, kw_v[...])
    loads["qw"].wait()
    query = dot(normed, qw_v[...])
    loads["vw"].wait()
    value = dot(normed, vw_v[...])

    both = jnp.concatenate([query, key], axis=0)
    wide = jnp.concatenate([key, query, jnp.zeros((LANES - 2 * tokens, key.shape[1]), f32)], axis=0)
    grams = dot(both, wide, ((1,), (1,)), HIGHEST)
    aux[r, :, pl.ds(0, vs)] = value
    aux[r, :, pl.ds(vs, LANES)] = grams[:tokens]
    aux[r, :, pl.ds(vs + LANES, LANES)] = grams[tokens:]
    pl.semaphore_wait(barrier, everyone - 1)
    aux_wait, aux_end = exchange(rows, r, lambda p: aux.at[r], aux, aux_s, aux_r, in_rows)

    loads["state"].wait()
    s_high, s_low = halves(state_v[...])
    b_high, b_low = halves(both)
    first = dot(jnp.concatenate([b_high, b_low], axis=0), s_high)
    found = first[:2 * tokens] + first[2 * tokens:] + dot(b_high, s_low)
    look[r] = found.astype(bf16)
    look_wait, look_end = exchange(rows, r, lambda p: look.at[r], look, look_s, look_r, in_rows)

    cw = voc_v.shape[1] // chunks
    vloads = []
    for c in range(chunks):
        at = pl.ds(c * cw, cw)
        vloads.append(pltpu.make_async_copy(vocab.at[:, at], voc_v.at[:, at], voc_sem.at[c]))
        vloads[-1].start()

    loads["gw"].wait()
    loads["rate"].wait()
    normed32 = normed.astype(f32)
    gate0 = jnp.sum(normed32 * gw_v[0:1, :].astype(f32), axis=1, keepdims=True)
    gate1 = jnp.sum(normed32 * gw_v[1:2, :].astype(f32), axis=1, keepdims=True)
    softplus = jnp.maximum(gate0, 0.0) + jnp.log1p(jnp.exp(-jnp.abs(gate0)))
    log_decay = -rate_v[...] * softplus
    strength = jax.nn.sigmoid(gate1)
    row = lax.broadcasted_iota(jnp.int32, (tokens, LANES), 0)
    col = lax.broadcasted_iota(jnp.int32, (tokens, LANES), 1)
    same = row == col
    causal = row >= col
    strictly = row > col

    def as_row(column):
        return jnp.sum(jnp.where(same, column, 0.0), axis=0, keepdims=True)

    reach = jnp.sum(jnp.where(causal, as_row(log_decay), 0.0), axis=1, keepdims=True)
    reach_row = as_row(reach)
    ratio = jnp.where(causal, jnp.exp(jnp.where(causal, reach - reach_row, 0.0)), 0.0)
    decay = jnp.exp(reach)
    last = reach[tokens - 1:tokens, :]
    loads["zw"].wait()
    zgate = dot(normed, zw_v[...])
    silu = zgate * jax.nn.sigmoid(zgate)

    aux_wait()
    gq = aux[0, :, pl.ds(vs, LANES)]
    gk = aux[0, :, pl.ds(vs + LANES, LANES)]
    for p in range(1, rows):
        gq += aux[p, :, pl.ds(vs, LANES)]
        gk += aux[p, :, pl.ds(vs + LANES, LANES)]
    values = jnp.concatenate([aux[p, :, pl.ds(0, vs)] for p in range(rows)], axis=1)
    dk = shape["dk"]
    k_len = jnp.sum(jnp.where(same, gk, 0.0), axis=1, keepdims=True)
    q_len = jnp.sum(jnp.where(col == row + tokens, gq, 0.0), axis=1, keepdims=True)
    k_scale = lax.rsqrt(k_len + epsilon)
    q_scale = lax.rsqrt(q_len + epsilon) * dk ** (-0.5)
    k_scale_row = as_row(k_scale)
    lower = jnp.where(strictly, strength * ratio * (gk * k_scale * k_scale_row), 0.0)
    cross = ratio * (gq * q_scale * k_scale_row)
    inverse = jnp.where(same, 1.0, 0.0)
    for i in range(tokens - 1):
        inverse = inverse - lower[:, i:i + 1] * inverse[i:i + 1, :]
    inverse = inverse[:, :tokens]
    reader = dot(cross[:, :tokens], inverse, precision=HIGHEST)
    solver = jnp.concatenate([inverse, reader], axis=0)

    look_wait()
    looked = look[0].astype(f32)
    for p in range(1, rows):
        looked += look[p].astype(f32)
    right = strength * (values - decay * k_scale * looked[tokens:])
    solved = dot(solver, right, precision=HIGHEST)
    updates = solved[:tokens]
    readouts = decay * q_scale * looked[:tokens] + solved[tokens:]
    read_v[...] = readouts
    norm = lax.rsqrt(jnp.mean(readouts * readouts, axis=-1, keepdims=True) + epsilon)
    piece = read_v[:, pl.ds(pl.multiple_of(r * vs, LANES), vs)]
    loads["ogain"].wait()
    gated = (piece * norm * ogain_v[...] * silu).astype(bf16)
    loads["ow"].wait()
    partial = dot(gated, ow_v[...])
    cut = width // group
    for p in range(group):
        parts[p] = partial[:, p * cut:(p + 1) * cut].astype(parts.dtype)
    rs_wait, rs_end = exchange(group, g, lambda p: parts.at[p], rs, rs_s, rs_r, in_group)
    rs[g] = parts[g]

    u_high, u_low = halves(jnp.exp(last - reach) * updates)
    k_high, k_low = halves(key * k_scale)
    ins = ((0,), (0,))
    grown = dot(k_high, u_high, ins) + dot(k_high, u_low, ins) + dot(k_low, u_high, ins)
    ns_v[...] = jnp.exp(last) * state_v[...] + grown
    ns_store = pltpu.make_async_copy(ns_v, new_state, out_sem.at[0])
    ns_store.start()

    rs_wait()
    mixed = rs[0].astype(f32)
    for p in range(1, group):
        mixed += rs[p].astype(f32)
    ag[g] = mixed.astype(ag.dtype)
    ag_wait, ag_end = exchange(group, g, lambda p: ag.at[g], ag, ag_s, ag_r, in_group)
    loads["fgain"].wait()
    ag_wait()
    stream = hid_v[...].astype(f32) + jnp.concatenate([ag[p].astype(f32) for p in range(group)], axis=1)
    fin[d] = (stream * lax.rsqrt(jnp.mean(stream * stream, axis=-1, keepdims=True) + epsilon) * fgain_v[...]).astype(bf16)
    fin_wait, fin_end = exchange(dps, d, lambda p: fin.at[d], fin, fin_s, fin_r, in_dp)
    fin_wait()
    final = fin[...].reshape(dps * tokens, width)
    for c in range(chunks):
        at = pl.ds(c * cw, cw)
        vloads[c].wait()
        log_v[:, at] = dot(final, voc_v[:, at])
    logits_store = pltpu.make_async_copy(log_v, logits_out, out_sem.at[1])
    logits_store.start()
    logits = log_v[...]
    peak = jnp.max(logits, axis=1, keepdims=True)
    total = jnp.sum(jnp.exp(logits - peak), axis=1, keepdims=True)
    scored, lanes = dps * tokens, stats.shape[2]
    diagonal = (lax.broadcasted_iota(jnp.int32, (scored, lanes), 0)
                == lax.broadcasted_iota(jnp.int32, (scored, lanes), 1))
    stats[me, 0:1, :] = jnp.sum(jnp.where(diagonal, peak, 0.0), axis=0, keepdims=True)
    stats[me, 1:2, :] = jnp.sum(jnp.where(diagonal, total, 0.0), axis=0, keepdims=True)
    st_wait, st_end = exchange(everyone, me, lambda p: stats.at[me], stats, st_s, st_r, anywhere)
    for end in (aux_end, look_end, rs_end, ag_end, fin_end):
        end()
    ns_store.wait()
    logits_store.wait()
    st_wait()
    peaks = stats[:, 0, :]
    sums = stats[:, 1, :]
    top = jnp.max(peaks, axis=0, keepdims=True)
    log_total = top + jnp.log(jnp.sum(sums * jnp.exp(peaks - top), axis=0, keepdims=True))
    tot_v[...] = jnp.broadcast_to(
        jnp.sum(jnp.where(diagonal, log_total, 0.0), axis=1, keepdims=True), tot_v.shape)
    tot_store = pltpu.make_async_copy(tot_v, total_out, out_sem.at[2])
    tot_store.start()
    st_end()
    tot_store.wait()


def on_device(shape, hidden, norm_gain, qw, kw, vw, zw, gw, rate, ogain, ow, state, fgain, vocab):
    seqs, tokens, width = hidden.shape
    assert seqs == 1 and hidden.shape[0] == state.shape[1] and norm_gain.shape[0] == 1
    dps, rows, heads = shape["dp"], shape["rows"], shape["heads"]
    group, everyone = rows * heads, dps * rows * heads
    ks, dv = state.shape[3:]
    vs, vl = vw.shape[2], vocab.shape[1]
    scored = dps * tokens
    lanes = -(-scored // LANES) * LANES
    chunks = max(1, vl // 512)
    shape = dict(shape, dk=ks * rows)
    args = (hidden[0], norm_gain, qw[0], kw[0], vw[0], zw[0], gw[0, :, :, 0], rate, ogain, ow[0],
            state[0, 0, 0], fgain.reshape(1, -1), vocab)
    dma = pltpu.SemaphoreType.DMA
    scratch = [pltpu.VMEM(a.shape, a.dtype) for a in args] + [
        pltpu.VMEM((rows, tokens, vs + 2 * LANES), f32),
        pltpu.VMEM((rows, 2 * tokens, dv), bf16),
        pltpu.VMEM((tokens, dv), f32),
        pltpu.VMEM((group, tokens, width // group), bf16),
        pltpu.VMEM((group, tokens, width // group), bf16),
        pltpu.VMEM((group, tokens, width // group), bf16),
        pltpu.VMEM((dps, tokens, width), bf16),
        pltpu.VMEM((everyone, 2, lanes), f32),
        pltpu.VMEM((ks, dv), f32),
        pltpu.VMEM((scored, vl), f32),
        pltpu.VMEM((scored, LANES), f32),
        dma((12,)), dma((chunks,)), dma((3,)),
    ] + [dma((n,)) for n in (rows, rows, rows, rows, group, group, group, group, dps, dps, everyone, everyone)]
    anywhere = pl.BlockSpec(memory_space=pl.ANY)
    new_state, logits, total = pl.pallas_call(
        functools.partial(kernel, shape, chunks),
        out_shape=(jax.ShapeDtypeStruct((ks, dv), f32), jax.ShapeDtypeStruct((scored, vl), f32),
                   jax.ShapeDtypeStruct((scored, LANES), f32)),
        in_specs=[anywhere] * len(args),
        out_specs=(anywhere,) * 3,
        scratch_shapes=scratch,
        compiler_params=pltpu.CompilerParams(
            collective_id=0, has_side_effects=True, vmem_limit_bytes=48 * 1024 * 1024),
    )(*args)
    log_probs = (logits - total[:, :1]).reshape(dps, tokens, vl)
    return new_state.reshape(state.shape), log_probs


def solution(mesh):
    in_specs = (
        P("dp", None, None),
        P(),
        P(None, None, ("heads", "rows")),
        P(None, None, ("heads", "rows")),
        P(None, None, ("heads", "rows")),
        P(None, None, ("heads", "rows")),
        P(None, None, None, "heads"),
        P(None, "heads"),
        P(None, "rows"),
        P(None, ("heads", "rows"), None),
        P(None, "dp", "heads", "rows", None),
        P(),
        P(None, ("dp", "rows", "heads")),
    )
    out_specs = (P(None, "dp", "heads", "rows", None), P(None, None, ("dp", "rows", "heads")))
    return jax.shard_map(functools.partial(on_device, dict(mesh.shape)), mesh=mesh, in_specs=in_specs,
                         out_specs=out_specs, check_vma=False)
```

```python
import functools

import jax
import jax.numpy as jnp
from jax import lax
from jax.experimental import pallas as pl
from jax.experimental.pallas import tpu as pltpu
from jax.sharding import PartitionSpec as P

MESH = pl.DeviceIdType.MESH
f32 = jnp.float32
bf16 = jnp.bfloat16
epsilon = 1e-06
HIGHEST = lax.Precision.HIGHEST
LANES = 128
LIMIT = 62 * 1024 * 1024


def halves(x):
    high = x.astype(bf16)
    return high, (x - high.astype(f32)).astype(bf16)


def dot(a, b, dims=((1,), (0,)), precision=None):
    return lax.dot_general(a, b, (dims, ((), ())), precision=precision, preferred_element_type=f32)


def looped(n, step):
    if n > 64:
        lax.fori_loop(1, n, step, 0)
    else:
        for k in range(1, n):
            step(k, 0)


def wrapped(a, n):
    return jnp.where(a >= n, a - n, a)


def exchange(n, me, src_of, dst, send, recv, device_of):
    def other(k):
        return wrapped(me + k, n)

    def outgoing(p):
        return pltpu.make_async_remote_copy(
            src_ref=src_of(p), dst_ref=dst.at[me], send_sem=send.at[p], recv_sem=recv.at[me],
            device_id=device_of(p), device_id_type=MESH)

    def incoming(p):
        return pltpu.make_async_remote_copy(
            src_ref=dst.at[p], dst_ref=dst.at[p], send_sem=send.at[p], recv_sem=recv.at[p],
            device_id=device_of(p), device_id_type=MESH)

    def over(act):
        def step(k, _):
            act(other(k))
            return 0

        looped(n, step)

    over(lambda p: outgoing(p).start())
    return (lambda: over(lambda p: incoming(p).wait_recv()),
            lambda: over(lambda p: outgoing(p).wait_send()))


def kernel(shape, chunks,
           hidden, norm_gain, qw, kw, vw, zw, gw, rate, ogain, ow, state, fgain, vocab,
           new_state, logits_out, total_out,
           hid_v, ngain_v, qw_v, kw_v, vw_v, zw_v, gw_v, rate_v, ogain_v, ow_v, state_v, fgain_v, voc_v,
           aux, look, read_v, parts, rs, ag, fin, stats, ns_v, log_v, tot_v,
           in_sem, voc_sem, out_sem,
           aux_s, aux_r, look_s, look_r, rs_s, rs_r, ag_s, ag_r, fin_s, fin_r, st_s, st_r):
    dps, rows, heads = shape["dp"], shape["rows"], shape["heads"]
    group = rows * heads
    everyone = dps * group
    d, r, h = (lax.axis_index(a) for a in ("dp", "rows", "heads"))
    g = r * heads + h
    me = d * group + g
    tokens, width = hid_v.shape
    vs = vw_v.shape[1]

    def in_group(p):
        return {"dp": d, "rows": lax.div(p, heads), "heads": lax.rem(p, heads)}

    def anywhere(p):
        q = lax.rem(p, group)
        return {"dp": lax.div(p, group), "rows": lax.div(q, heads), "heads": lax.rem(q, heads)}

    def in_rows(p):
        return {"dp": d, "rows": p, "heads": h}

    def in_dp(p):
        return {"dp": p, "rows": r, "heads": h}

    loads = {}
    order = (("hid", hidden, hid_v), ("ngain", norm_gain, ngain_v), ("kw", kw, kw_v), ("qw", qw, qw_v),
             ("vw", vw, vw_v), ("state", state, state_v), ("gw", gw, gw_v), ("rate", rate, rate_v),
             ("zw", zw, zw_v), ("ogain", ogain, ogain_v), ("fgain", fgain, fgain_v), ("ow", ow, ow_v))
    for i, (name, src, dst) in enumerate(order):
        loads[name] = pltpu.make_async_copy(src, dst, in_sem.at[i])
        loads[name].start()
    barrier = pltpu.get_barrier_semaphore()

    def greet(k, _):
        pl.semaphore_signal(barrier, inc=1, device_id=anywhere(wrapped(me + k, everyone)), device_id_type=MESH)
        return 0

    looped(everyone, greet)

    loads["hid"].wait()
    loads["ngain"].wait()
    stream = hid_v[...].astype(f32)
    normed = (stream * lax.rsqrt(jnp.mean(stream * stream, axis=-1, keepdims=True) + epsilon) * ngain_v[...]).astype(bf16)
    loads["kw"].wait()
    key = dot(normed, kw_v[...])
    loads["qw"].wait()
    query = dot(normed, qw_v[...])
    loads["vw"].wait()
    value = dot(normed, vw_v[...])

    both = jnp.concatenate([query, key], axis=0)
    rest = jnp.zeros((LANES - 3 * tokens, key.shape[1]), f32)
    none = jnp.zeros_like(key)
    lanes_in = ((1,), (1,))
    grams = (dot(key, jnp.concatenate([key, none, none, rest], axis=0), lanes_in, HIGHEST)
             + dot(query, jnp.concatenate([none, key, query, rest], axis=0), lanes_in, HIGHEST))
    aux[r, :, pl.ds(0, vs)] = value
    aux[r, :, pl.ds(vs, LANES)] = grams
    pl.semaphore_wait(barrier, everyone - 1)
    aux_wait, aux_end = exchange(rows, r, lambda p: aux.at[r], aux, aux_s, aux_r, in_rows)

    loads["state"].wait()
    s_high, s_low = halves(state_v[...])
    b_high, b_low = halves(both)
    first = dot(jnp.concatenate([b_high, b_low], axis=0), s_high)
    found = first[:2 * tokens] + first[2 * tokens:] + dot(b_high, s_low)
    look[r] = found.astype(bf16)
    look_wait, look_end = exchange(rows, r, lambda p: look.at[r], look, look_s, look_r, in_rows)

    cw = voc_v.shape[1] // chunks
    vloads = []
    for c in range(chunks):
        at = pl.ds(c * cw, cw)
        vloads.append(pltpu.make_async_copy(vocab.at[:, at], voc_v.at[:, at], voc_sem.at[c]))
        vloads[-1].start()

    loads["gw"].wait()
    loads["rate"].wait()
    normed32 = normed.astype(f32)
    gate0 = jnp.sum(normed32 * gw_v[0:1, :].astype(f32), axis=1, keepdims=True)
    gate1 = jnp.sum(normed32 * gw_v[1:2, :].astype(f32), axis=1, keepdims=True)
    softplus = jnp.maximum(gate0, 0.0) + jnp.log1p(jnp.exp(-jnp.abs(gate0)))
    log_decay = -rate_v[...] * softplus
    strength = jax.nn.sigmoid(gate1)
    row = lax.broadcasted_iota(jnp.int32, (tokens, LANES), 0)
    col = lax.broadcasted_iota(jnp.int32, (tokens, LANES), 1)
    same = row == col
    causal = row >= col
    strictly = row > col

    def as_row(column):
        return jnp.sum(jnp.where(same, column, 0.0), axis=0, keepdims=True)

    reach = jnp.sum(jnp.where(causal, as_row(log_decay), 0.0), axis=1, keepdims=True)
    reach_row = as_row(reach)
    ratio = jnp.where(causal, jnp.exp(jnp.where(causal, reach - reach_row, 0.0)), 0.0)
    decay = jnp.exp(reach)
    last = reach[tokens - 1:tokens, :]
    loads["zw"].wait()
    zgate = dot(normed, zw_v[...])
    silu = zgate * jax.nn.sigmoid(zgate)

    aux_wait()
    gk = aux[0, :, pl.ds(vs, LANES)]
    for p in range(1, rows):
        gk += aux[p, :, pl.ds(vs, LANES)]
    values = jnp.concatenate([aux[p, :, pl.ds(0, vs)] for p in range(rows)], axis=1)
    dk = shape["dk"]
    k_len = jnp.sum(jnp.where(same, gk, 0.0), axis=1, keepdims=True)
    q_len = jnp.sum(jnp.where(col == row + 2 * tokens, gk, 0.0), axis=1, keepdims=True)
    k_scale = lax.rsqrt(k_len + epsilon)
    q_scale = lax.rsqrt(q_len + epsilon) * dk ** (-0.5)
    k_scale_row = as_row(k_scale)
    lower = jnp.where(strictly, strength * ratio * (gk * k_scale * k_scale_row), 0.0)
    cross = ratio[:, :tokens] * (gk[:, tokens:2 * tokens] * q_scale * k_scale_row[:, :tokens])
    inverse = jnp.where(same, 1.0, 0.0)
    for i in range(tokens - 1):
        inverse = inverse - lower[:, i:i + 1] * inverse[i:i + 1, :]
    inverse = inverse[:, :tokens]
    reader = dot(cross, inverse, precision=HIGHEST)
    solver = jnp.concatenate([inverse, reader], axis=0)

    look_wait()
    looked = look[0].astype(f32)
    for p in range(1, rows):
        looked += look[p].astype(f32)
    right = strength * (values - decay * k_scale * looked[tokens:])
    solved = dot(solver, right, precision=HIGHEST)
    updates = solved[:tokens]
    readouts = decay * q_scale * looked[:tokens] + solved[tokens:]
    read_v[...] = readouts
    norm = lax.rsqrt(jnp.mean(readouts * readouts, axis=-1, keepdims=True) + epsilon)
    piece = read_v[:, pl.ds(pl.multiple_of(r * vs, LANES), vs)]
    loads["ogain"].wait()
    gated = (piece * norm * ogain_v[...] * silu).astype(bf16)
    loads["ow"].wait()
    partial = dot(gated, ow_v[...])
    cut = width // group
    for p in range(group):
        parts[p] = partial[:, p * cut:(p + 1) * cut].astype(parts.dtype)
    rs_wait, rs_end = exchange(group, g, lambda p: parts.at[p], rs, rs_s, rs_r, in_group)
    rs[g] = parts[g]

    u_high, u_low = halves(jnp.exp(last - reach) * updates)
    k_high, k_low = halves(key * k_scale)
    ins = ((0,), (0,))
    grown = dot(k_high, u_high, ins) + dot(k_high, u_low, ins) + dot(k_low, u_high, ins)
    ns_v[...] = jnp.exp(last) * state_v[...] + grown
    ns_store = pltpu.make_async_copy(ns_v, new_state, out_sem.at[0])
    ns_store.start()

    rs_wait()
    mixed = rs[0].astype(f32)
    for p in range(1, group):
        mixed += rs[p].astype(f32)
    ag[g] = mixed.astype(ag.dtype)
    ag_wait, ag_end = exchange(group, g, lambda p: ag.at[g], ag, ag_s, ag_r, in_group)
    loads["fgain"].wait()
    ag_wait()
    stream = hid_v[...].astype(f32) + jnp.concatenate([ag[p].astype(f32) for p in range(group)], axis=1)
    fin[d] = (stream * lax.rsqrt(jnp.mean(stream * stream, axis=-1, keepdims=True) + epsilon) * fgain_v[...]).astype(bf16)
    fin_wait, fin_end = exchange(dps, d, lambda p: fin.at[d], fin, fin_s, fin_r, in_dp)
    fin_wait()
    final = fin[...].reshape(dps * tokens, width)
    for c in range(chunks):
        at = pl.ds(c * cw, cw)
        vloads[c].wait()
        log_v[:, at] = dot(final, voc_v[:, at])
    logits_store = pltpu.make_async_copy(log_v, logits_out, out_sem.at[1])
    logits_store.start()
    logits = log_v[...]
    peak = jnp.max(logits, axis=1, keepdims=True)
    total = jnp.sum(jnp.exp(logits - peak), axis=1, keepdims=True)
    scored, lanes = dps * tokens, stats.shape[2]
    diagonal = (lax.broadcasted_iota(jnp.int32, (scored, lanes), 0)
                == lax.broadcasted_iota(jnp.int32, (scored, lanes), 1))
    stats[me, 0:1, :] = jnp.sum(jnp.where(diagonal, peak, 0.0), axis=0, keepdims=True)
    stats[me, 1:2, :] = jnp.sum(jnp.where(diagonal, total, 0.0), axis=0, keepdims=True)
    st_wait, st_end = exchange(everyone, me, lambda p: stats.at[me], stats, st_s, st_r, anywhere)
    for end in (aux_end, look_end, rs_end, ag_end, fin_end):
        end()
    ns_store.wait()
    logits_store.wait()
    st_wait()
    peaks = stats[:, 0, :]
    sums = stats[:, 1, :]
    top = jnp.max(peaks, axis=0, keepdims=True)
    log_total = top + jnp.log(jnp.sum(sums * jnp.exp(peaks - top), axis=0, keepdims=True))
    tot_v[...] = jnp.broadcast_to(
        jnp.sum(jnp.where(diagonal, log_total, 0.0), axis=1, keepdims=True), tot_v.shape)
    tot_store = pltpu.make_async_copy(tot_v, total_out, out_sem.at[2])
    tot_store.start()
    st_end()
    tot_store.wait()


def finish(state_in, logits_in, total_in, state_out, log_probs_out, state, logits, total, sem_in, sem_out):
    pieces = sem_in.shape[0] - 2
    depth = state.shape[0] // pieces
    half = logits.shape[1] // 2
    loads = [pltpu.make_async_copy(logits_in, logits, sem_in.at[pieces]),
             pltpu.make_async_copy(total_in, total, sem_in.at[pieces + 1])]
    stores = []
    for i in range(pieces):
        at = pl.ds(i * depth, depth)
        loads.append(pltpu.make_async_copy(state_in.at[at], state.at[at], sem_in.at[i]))
        stores.append(pltpu.make_async_copy(state.at[at], state_out.at[at], sem_out.at[i]))
    for copy in loads:
        copy.start()
    loads[0].wait()
    loads[1].wait()
    for i in range(2):
        at = pl.ds(i * half, half)
        logits[:, at] = logits[:, at] - total[:, 0:1]
        stores.append(pltpu.make_async_copy(logits.at[:, at], log_probs_out.at[:, at], sem_out.at[pieces + i]))
        stores[-1].start()
    for i in range(pieces):
        loads[2 + i].wait()
        stores[i].start()
    for store in stores:
        store.wait()


def on_device(shape, hidden, norm_gain, qw, kw, vw, zw, gw, rate, ogain, ow, state, fgain, vocab):
    seqs, tokens, width = hidden.shape
    assert seqs == 1 and hidden.shape[0] == state.shape[1] and norm_gain.shape[0] == 1
    dps, rows, heads = shape["dp"], shape["rows"], shape["heads"]
    group, everyone = rows * heads, dps * rows * heads
    ks, dv = state.shape[3:]
    vs, vl = vw.shape[2], vocab.shape[1]
    scored = dps * tokens
    lanes = -(-scored // LANES) * LANES
    chunks = max(1, vl // 512)
    shape = dict(shape, dk=ks * rows)
    args = (hidden[0], norm_gain, qw[0], kw[0], vw[0], zw[0], gw[0, :, :, 0], rate, ogain, ow[0],
            state[0, 0, 0], fgain.reshape(1, -1), vocab)
    dma = pltpu.SemaphoreType.DMA
    scratch = [pltpu.VMEM(a.shape, a.dtype) for a in args] + [
        pltpu.VMEM((rows, tokens, vs + LANES), f32),
        pltpu.VMEM((rows, 2 * tokens, dv), bf16),
        pltpu.VMEM((tokens, dv), f32),
        pltpu.VMEM((group, tokens, width // group), bf16),
        pltpu.VMEM((group, tokens, width // group), bf16),
        pltpu.VMEM((group, tokens, width // group), bf16),
        pltpu.VMEM((dps, tokens, width), bf16),
        pltpu.VMEM((everyone, 2, lanes), f32),
        pltpu.VMEM((ks, dv), f32),
        pltpu.VMEM((scored, vl), f32),
        pltpu.VMEM((scored, LANES), f32),
        dma((12,)), dma((chunks,)), dma((3,)),
    ] + [dma((n,)) for n in (rows, rows, rows, rows, group, group, group, group, dps, dps, everyone, everyone)]
    in_hbm = pl.BlockSpec(memory_space=pltpu.HBM)
    anyplace = pl.BlockSpec(memory_space=pl.ANY)
    results = pl.pallas_call(
        functools.partial(kernel, shape, chunks),
        out_shape=(jax.ShapeDtypeStruct((ks, dv), f32), jax.ShapeDtypeStruct((scored, vl), f32),
                   jax.ShapeDtypeStruct((scored, LANES), f32)),
        in_specs=[in_hbm] * len(args),
        out_specs=(anyplace,) * 3,
        scratch_shapes=scratch,
        compiler_params=pltpu.CompilerParams(
            collective_id=0, has_side_effects=True, vmem_limit_bytes=LIMIT),
    )(*args)
    new_state, log_probs = pl.pallas_call(
        finish,
        out_shape=(jax.ShapeDtypeStruct((ks, dv), f32), jax.ShapeDtypeStruct((scored, vl), f32)),
        in_specs=[anyplace] * 3,
        out_specs=(anyplace,) * 2,
        scratch_shapes=[pltpu.VMEM((ks, dv), f32), pltpu.VMEM((scored, vl), f32),
                        pltpu.VMEM((scored, LANES), f32), dma((6,)), dma((6,))],
        compiler_params=pltpu.CompilerParams(vmem_limit_bytes=LIMIT),
    )(*results)
    return new_state.reshape(state.shape), log_probs.reshape(dps, tokens, vl)


def solution(mesh):
    in_specs = (
        P("dp", None, None),
        P(),
        P(None, None, ("heads", "rows")),
        P(None, None, ("heads", "rows")),
        P(None, None, ("heads", "rows")),
        P(None, None, ("heads", "rows")),
        P(None, None, None, "heads"),
        P(None, "heads"),
        P(None, "rows"),
        P(None, ("heads", "rows"), None),
        P(None, "dp", "heads", "rows", None),
        P(),
        P(None, ("dp", "rows", "heads")),
    )
    out_specs = (P(None, "dp", "heads", "rows", None), P(None, None, ("dp", "rows", "heads")))
    return jax.shard_map(functools.partial(on_device, dict(mesh.shape)), mesh=mesh, in_specs=in_specs,
                         out_specs=out_specs, check_vma=False)
```
